32 devices in a mesh: gx: 2 (over x), gy: 4 (over z), gz: 4 (over y, core).
Axes of the slice: x: 2, y: 2, z: 4, core: 2. Of those that a mesh axis runs over, the one named last changes fastest.
Arguments:
- particle_mass: float32 [1048576], P(('gx', 'gy', 'gz')), may hold values from 0.5 to 2
- particle_velocity: float32 [3, 1048576], P(None, ('gx', 'gy', 'gz')), may hold values from -6 to 6
- particle_affine: float32 [9, 1048576], P(None, ('gx', 'gy', 'gz')), may hold values from -6 to 6
- particle_cell: int32 [3, 1048576], P(None, ('gx', 'gy', 'gz')), may hold values from 0 to 13
- particle_fraction: int32 [3, 1048576], P(None, ('gx', 'gy', 'gz')), may hold values from 0 to 1023
- block_owner: int32 [2048, 1], P(('gx', 'gy', 'gz')), may hold values from 0 to 15; in each aligned block of 64 rows (0 to 63, 64 to 127, ...) at most 8 rows name the same one
- block_slot: int32 [2048], P(('gx', 'gy', 'gz')), may hold values from 0 to 31
- block_count: int32 [2048], P(('gx', 'gy', 'gz')), may hold values from 128 to 512
- cell_drag: float32 [1024, 4096], P(('gx', 'gy', 'gz')), may hold values from 0.5 to 2
Outputs:
- grid_velocity: float32 [1024, 3, 4096], P(('gx', 'gy', 'gz'))
- new_velocity: float32 [3, 1048576], P(None, ('gx', 'gy', 'gz'))
- new_affine: float32 [9, 1048576], P(None, ('gx', 'gy', 'gz'))
The draws below stay inside these ranges and needn't reach their ends.
Inputs may be any that keep to these rules, and one draw needn't show every extreme that they name: `block_owner`: owner index counted over the devices with the particle device's own gx index, in gy+gz order; among the rows of one device, no owner is named more than 8 times. `block_count`: slots at or beyond the count are absent. `particle_cell`: A particle's three stencil nodes lie inside its grid block.
All inputs are finite; a program needn't handle non-finite values.
Results may differ from the reference program's by a relative error of at most 0.0085.
Values may be sent and summed in bfloat16 or wider, within the bound.
A program may use at most 128 MiB of HBM per device.

```python
import math
import jax
import jax.numpy as jnp
import numpy as np
from jax import lax

EDGE = 16
PB = 512
QUANT = 1024
BLK_DEV = 64
GROUP = 16
CAP = 8
TILES_DEV = 32
BLOCKS = 2048
PARTICLES = 1048576
TILES = 1024
CELLS = 4096
N_GY = 4
N_GZ = 4


def place_ends(entries, key, smallest, high):
    longest = entries.shape.index(max(entries.shape))
    spots = []
    for shift in (0, 1):
        where = [jax.random.randint(jax.random.fold_in(key, axis), (), 0, length) for axis, length in enumerate(entries.shape)]
        where[longest] = (where[longest] + shift) % entries.shape[longest]
        spots.append(tuple(where))
    return entries.at[spots[0]].set(smallest).at[spots[1]].set(high)


def block_levels(own_key, dims, shards, low, largest):
    def one(axis_at, blocks):
        heights = jax.random.uniform(jax.random.fold_in(jax.random.fold_in(own_key, 6), axis_at), (blocks,), jnp.float32, low / len(shards), largest / len(shards))
        return jnp.repeat(jnp.exp(heights), dims[axis_at] // blocks).reshape((-1,) + (1,) * (len(dims) - axis_at - 1))

    loudness = one(*shards[0])
    for cut in shards[1:]:
        loudness = loudness * one(*cut)
    return loudness


def shared_out(stream_key, own, number, rows, amount, top, most, slope):
    order = jax.random.permutation(stream_key, amount)
    packed, common = load_shares(amount, rows * top, most, slope, True), load_shares(amount, rows * top, most, slope, False)
    places = jnp.arange(amount)

    def named(lengths, rotation):
        used = int((lengths > 0).sum())
        fixed = max(1, used // 4)
        shifted = fixed + (places - fixed + rotation * (used - fixed)) % max(1, amount - fixed)
        return jnp.zeros((amount,), jnp.int32).at[order[jnp.where(places < fixed, places, shifted)]].set(jnp.asarray(lengths, jnp.int32))

    lengths = jnp.where(number % 4 == 0, named(packed, number // 4), named(common, number - number // 4 - 1))
    mixed = jax.random.permutation(jax.random.fold_in(own, 3), amount)
    giver, receiver = mixed[0:amount // 2 * 2:2], mixed[1:amount // 2 * 2:2]
    margin = jnp.minimum(lengths[giver] - 1, most - lengths[receiver]) // 2
    margin = jnp.where((giver == order[0]) | (receiver == order[0]) | (lengths[receiver] == 0), 0, jnp.maximum(margin, 0))
    shifted = jax.random.randint(jax.random.fold_in(own, 4), (amount // 2,), 0, 1 << 20) % (margin + 1)
    lengths = lengths.at[giver].add(-shifted).at[receiver].add(shifted)
    labels = jnp.searchsorted(jnp.cumsum(lengths), jnp.arange(rows * top), side="right").astype(jnp.int32)
    table = labels.reshape(top, rows).T
    table = table[jax.random.permutation(jax.random.fold_in(own, 1), rows)]
    rotation = jax.random.randint(jax.random.fold_in(own, 2), (rows, 1), 0, top)
    return jnp.take_along_axis(table, (jnp.arange(top)[None, :] + rotation) % top, axis=1)


def load_shares(amount, total, bound, slope, full):
    loads = [(1 << 20) // math.isqrt(standing ** slope) + 1 for standing in range(1, amount + 1)]
    largest = bound if full else min(bound, max(-(-total // amount), total * loads[0] // sum(loads)))
    least = 1 if total - largest >= amount - 1 else 0
    holding, rest = [largest] + [least] * (amount - 1), total - largest - least * (amount - 1)
    while rest > 0:
        free = [i for i in range(1, amount) if holding[i] < largest] or [i for i in range(1, amount) if holding[i] < bound]
        whole, budget = sum([loads[i] for i in free]), rest
        for i in free:
            more = min(bound - holding[i], max(1, budget * loads[i] // whole), rest)
            holding[i] = holding[i] + more
            rest = rest - more
    return np.array(holding)


def gaussian(stream_key, extent, deviation, reach, pieces=(), kind=jnp.bfloat16):
    result = deviation * jax.random.normal(stream_key, extent, jnp.float32)
    if pieces:
        result = result * block_levels(stream_key, extent, pieces, -0.22, 0.18)
    return jnp.clip(result, -reach, reach).astype(kind)


def setup_inputs(seed: int = 0) -> dict:
    keys = jax.random.split(jax.random.key(seed), 10)
    particle_mass = jnp.clip(jnp.exp(math.log(2.0) - 1.3862944 * jax.random.uniform(keys[0], (PARTICLES,), jnp.float32) ** block_levels(keys[0], (PARTICLES,), ((0, 32),), -0.2, 0.2)), 0.5, 2.0)
    particle_velocity = gaussian(keys[1], (3, PARTICLES), 1.0, 6.0, ((1, 32),), jnp.float32)
    particle_affine = gaussian(keys[2], (9, PARTICLES), 1.0, 6.0, ((1, 32),), jnp.float32)
    particle_cell = place_ends(jax.random.randint(keys[3], (3, PARTICLES), 0, EDGE - 2), jax.random.fold_in(keys[3], 1), 0, (EDGE - 2) - 1).astype(jnp.int32)
    particle_fraction = place_ends(jax.random.randint(keys[4], (3, PARTICLES), 0, QUANT), jax.random.fold_in(keys[4], 1), 0, QUANT - 1).astype(jnp.int32)
    block_owner_keys = jax.random.split(jax.random.fold_in(keys[5], 1), BLOCKS // BLK_DEV)
    block_owner_turns = jax.random.permutation(jax.random.fold_in(keys[5], 3), BLOCKS // BLK_DEV)
    block_owner = jax.vmap(lambda own, number: shared_out(jax.random.fold_in(keys[5], 2), own, number, BLK_DEV, GROUP, 1, CAP, 2))(block_owner_keys, block_owner_turns).reshape((BLOCKS, 1))
    block_slot = place_ends(jax.random.randint(keys[6], (BLOCKS,), 0, TILES_DEV), jax.random.fold_in(keys[6], 1), 0, TILES_DEV - 1).astype(jnp.int32)
    block_count = place_ends(jax.random.randint(keys[7], (BLOCKS,), PB // 4, PB + 1), jax.random.fold_in(keys[7], 1), PB // 4, PB).astype(jnp.int32)
    cell_drag = jnp.clip(jnp.exp(math.log(2.0) - 1.3862944 * jax.random.uniform(keys[8], (TILES, CELLS), jnp.float32) ** block_levels(keys[8], (TILES, CELLS), ((0, 32),), -0.2, 0.2)), 0.5, 2.0)
    return dict(particle_mass=particle_mass, particle_velocity=particle_velocity, particle_affine=particle_affine, particle_cell=particle_cell, particle_fraction=particle_fraction, block_owner=block_owner, block_slot=block_slot, block_count=block_count, cell_drag=cell_drag)


def spline(offset):
    magnitude = jnp.abs(offset)
    inner_part = 0.75 - magnitude * magnitude
    outer_part = 0.5 * (1.5 - magnitude) * (1.5 - magnitude)
    return jnp.where(magnitude < 0.5, inner_part, jnp.where(magnitude < 1.5, outer_part, 0.0))


def particle_table(particle_mass, particle_velocity, particle_affine, particle_cell, particle_fraction, block_count):
    blocks = block_count.shape[0]
    batch_shape = (blocks, particle_mass.shape[0] // blocks)
    places = jnp.arange(batch_shape[1], dtype=jnp.int32)
    present = places[None, :] < block_count[:, None]
    live_mass = jnp.where(present, particle_mass.reshape(batch_shape), 0.0)
    position = particle_cell.astype(jnp.float32) + 0.5 + (particle_fraction.astype(jnp.float32) + 0.5) / QUANT
    return jnp.concatenate([live_mass[None], particle_velocity.reshape((3,) + batch_shape), particle_affine.reshape((9,) + batch_shape), position.reshape((3,) + batch_shape)], axis=0)


def stencil(particle_data):
    node_coords = jnp.arange(EDGE, dtype=jnp.float32)
    offset = node_coords[None, :, None, None] - particle_data[13:16][:, None]
    weights = spline(offset)
    return weights, weights * offset


def planes(weights, slopes):
    def outer(first_factor, second_factor):
        product_table = first_factor[:, None] * second_factor[None, :]
        return product_table.reshape((EDGE * EDGE,) + product_table.shape[2:]).astype(jnp.bfloat16)
    return outer(weights[1], weights[2]), outer(slopes[1], weights[2]), outer(weights[1], slopes[2])


def deposit(particle_data):
    batch_shape = particle_data.shape[1:]
    weights, slopes = stencil(particle_data)
    plane_zero, plane_one, plane_two = planes(weights, slopes)
    live_mass = particle_data[0]
    along_x = weights[0]
    slope_x = slopes[0]
    affine = particle_data[4:13].reshape((3, 3) + batch_shape)
    mass_lead = (live_mass[None] * along_x)[None]
    momentum_lead = live_mass[None, None] * (particle_data[1:4][:, None] * along_x[None] + affine[:, 0][:, None] * slope_x[None])
    lead_zero = jnp.concatenate([mass_lead, momentum_lead], axis=0).astype(jnp.bfloat16)
    lead_one = (live_mass[None, None] * affine[:, 1][:, None] * along_x[None]).astype(jnp.bfloat16)
    lead_two = (live_mass[None, None] * affine[:, 2][:, None] * along_x[None]).astype(jnp.bfloat16)

    def contract(lead, plane):
        flattened = lead.reshape((-1,) + batch_shape).astype(jnp.float32)
        return jnp.einsum("anp,bnp->nab", flattened, plane.astype(jnp.float32), precision=lax.Precision.HIGHEST)

    count_blocks = batch_shape[0]
    dep_zero = contract(lead_zero, plane_zero).reshape(count_blocks, 4, -1)
    dep_one = contract(lead_one, plane_one).reshape(count_blocks, 3, -1)
    dep_two = contract(lead_two, plane_two).reshape(count_blocks, 3, -1)
    return jnp.concatenate([dep_zero[:, :1], dep_zero[:, 1:] + dep_one + dep_two], axis=1)


def interpolate(particle_data, grid_rows):
    batch_shape = particle_data.shape[1:]
    weights, slopes = stencil(particle_data)
    plane_zero, plane_one, plane_two = planes(weights, slopes)
    along_x = weights[0]
    slope_x = slopes[0]
    flattened = grid_rows.reshape(batch_shape[0], 3 * EDGE, EDGE * EDGE).astype(jnp.float32)

    def contract(plane):
        moment = jnp.einsum("nab,bnp->anp", flattened, plane.astype(jnp.float32), precision=lax.Precision.HIGHEST)
        return moment.reshape((3, EDGE) + batch_shape)

    moment_zero = contract(plane_zero)
    moment_one = contract(plane_one)
    moment_two = contract(plane_two)
    velocity_out = jnp.sum(along_x[None] * moment_zero, axis=1)
    column_zero = 4.0 * jnp.sum(slope_x[None] * moment_zero, axis=1)
    column_one = 4.0 * jnp.sum(along_x[None] * moment_one, axis=1)
    column_two = 4.0 * jnp.sum(along_x[None] * moment_two, axis=1)
    affine_out = jnp.stack([column_zero, column_one, column_two], axis=1).reshape((9,) + batch_shape)
    present = (particle_data[0] > 0.0).astype(jnp.float32)
    return jnp.concatenate([velocity_out, affine_out], axis=0) * present[None]


def reference(particle_mass, particle_velocity, particle_affine, particle_cell, particle_fraction, block_owner, block_slot, block_count, cell_drag):
    group_size = N_GY * N_GZ
    particle_data = particle_table(particle_mass, particle_velocity, particle_affine, particle_cell, particle_fraction, block_count)
    blocks = block_count.shape[0]
    device = jnp.arange(blocks, dtype=jnp.int32) // BLK_DEV
    tile_ids = (((device // group_size) * group_size + block_owner[:, 0]) * TILES_DEV + block_slot).astype(jnp.int32)

    def accumulate(grid_sums, block_index):
        portion = lax.dynamic_slice_in_dim(particle_data, block_index, 1, 1)
        return grid_sums.at[tile_ids[block_index]].add(deposit(portion)[0]), None

    initial = jnp.zeros((cell_drag.shape[0], 4, cell_drag.shape[1]), jnp.float32)
    grid_sums = lax.scan(accumulate, initial, jnp.arange(blocks, dtype=jnp.int32))[0]
    grid_velocity = grid_sums[:, 1:] / (grid_sums[:, :1] + cell_drag[:, None, :])
    rounded = grid_velocity.astype(jnp.bfloat16)

    def sample(block_index):
        portion = lax.dynamic_slice_in_dim(particle_data, block_index, 1, 1)
        cell_rows = lax.dynamic_index_in_dim(rounded, tile_ids[block_index], 0, keepdims=True)
        return interpolate(portion, cell_rows)[:, 0]

    finished = lax.map(sample, jnp.arange(blocks, dtype=jnp.int32))
    finished = jnp.transpose(finished, (1, 0, 2)).reshape(12, -1)
    return grid_velocity, finished[:3], finished[3:]
```

```python
import functools

import jax
import jax.numpy as jnp
from jax import lax
from jax.experimental import pallas as pl
from jax.experimental.pallas import tpu as pltpu
from jax.sharding import PartitionSpec as P

EDGE = 16
QUANT = 1024
LANES = 128
FIELDS = 20
RESULTS = 12
UNROLL = 2
GROUP_AXES = ("gy", "gz")
F32 = jnp.float32
BF16 = jnp.bfloat16


def pack_kernel(
    capacity,
    owner_ref,
    slot_ref,
    count_ref,
    mass_ref,
    velocity_ref,
    affine_ref,
    cell_ref,
    fraction_ref,
    payload_ref,
    tiles_ref,
    dest_ref,
    used_ref,
    stage_ref,
):
    blocks = owner_ref.shape[0]
    slots = payload_ref.shape[0]
    width = mass_ref.shape[1]

    def clear_used(i, carry):
        used_ref[i] = 0
        return carry

    lax.fori_loop(0, used_ref.shape[0], clear_used, 0)

    def clear_tiles(i, carry):
        tiles_ref[i] = -1
        return carry

    lax.fori_loop(0, slots, clear_tiles, 0)

    lane = lax.broadcasted_iota(jnp.int32, (1, width), 1)

    def pack(block, carry):
        owner = owner_ref[block]
        rank = used_ref[owner]
        used_ref[owner] = rank + 1
        where = owner * capacity + rank
        dest_ref[block] = where
        tiles_ref[where] = slot_ref[block]
        cols = pl.ds(pl.multiple_of(block * width, LANES), width)
        live = jnp.where(lane < count_ref[block], mass_ref[pl.ds(block, 1), :], 0.0)
        velocity = velocity_ref[:, cols]
        affine = affine_ref[:, cols]
        code = cell_ref[:, cols] * QUANT + fraction_ref[:, cols]
        high = (code >> 7).astype(F32)
        low = (code & 127).astype(F32)
        for q in range(width // LANES):
            part = slice(q * LANES, (q + 1) * LANES)
            base = q * FIELDS
            stage_ref[base : base + 1] = live[:, part]
            stage_ref[base + 1 : base + 4] = velocity[:, part]
            stage_ref[base + 4 : base + 13] = affine[:, part]
            stage_ref[base + 13 : base + 16] = high[:, part]
            stage_ref[base + 16 : base + 19] = low[:, part]
        payload_ref[where] = stage_ref[...].astype(BF16)
        return carry

    lax.fori_loop(0, blocks, pack, 0)


def pack(capacity, slots, group_size, owner, slot, count, mass, velocity, affine, cell, fraction):
    blocks = owner.shape[0]
    width = mass.shape[0] // blocks
    rows = width // LANES * FIELDS
    smem = pl.BlockSpec(memory_space=pltpu.SMEM)
    vmem = pl.BlockSpec(memory_space=pltpu.VMEM)
    return pl.pallas_call(
        functools.partial(pack_kernel, capacity),
        name="pack",
        out_shape=(
            jax.ShapeDtypeStruct((slots, rows, LANES), BF16),
            jax.ShapeDtypeStruct((slots,), jnp.int32),
            jax.ShapeDtypeStruct((blocks,), jnp.int32),
        ),
        in_specs=[smem] * 3 + [vmem] * 5,
        out_specs=(vmem, smem, smem),
        scratch_shapes=[pltpu.SMEM((group_size,), jnp.int32), pltpu.VMEM((rows, LANES), F32)],
        compiler_params=pltpu.CompilerParams(vmem_limit_bytes=48 << 20),
    )(owner, slot, count, mass.reshape(blocks, width), velocity, affine, cell, fraction)


def spread(rows, field):
    quarters = rows.shape[0] // FIELDS
    return jnp.concatenate(
        [
            jnp.broadcast_to(rows[q * FIELDS + field : q * FIELDS + field + 1], (EDGE, LANES))
            for q in range(quarters)
        ],
        axis=1,
    )


def stencil(rows, node, dim):
    position = (
        spread(rows, 13 + dim) * (128.0 / QUANT)
        + spread(rows, 16 + dim) * (1.0 / QUANT)
        + (0.5 + 0.5 / QUANT)
    )
    offset = node - position
    magnitude = jnp.abs(offset)
    outer_part = jnp.maximum(1.5 - magnitude, 0.0)
    weight = jnp.where(
        magnitude < 0.5, 0.75 - magnitude * magnitude, 0.5 * outer_part * outer_part
    )
    return weight, weight * offset


def outer(first, second):
    table = first[:, None, :] * second[None, :, :]
    return table.reshape(EDGE * EDGE, first.shape[1])


def planes(rows, node):
    weight_y, slope_y = stencil(rows, node, 1)
    weight_z, slope_z = stencil(rows, node, 2)
    weight_y, slope_y = weight_y.astype(BF16), slope_y.astype(BF16)
    weight_z, slope_z = weight_z.astype(BF16), slope_z.astype(BF16)
    return outer(weight_y, weight_z), outer(slope_y, weight_z), outer(weight_y, slope_z)


def contract(lead, plane):
    return lax.dot_general(lead, plane, (((1,), (1,)), ((), ())), preferred_element_type=F32)


def deposit(rows):
    width = rows.shape[0] // FIELDS * LANES
    node = lax.broadcasted_iota(jnp.int32, (EDGE, width), 0).astype(F32)
    weight_x, slope_x = stencil(rows, node, 0)
    plane_zero, plane_one, plane_two = planes(rows, node)
    mass_x = spread(rows, 0) * weight_x
    mass_slope = spread(rows, 0) * slope_x
    lead_zero, lead_one, lead_two = [mass_x], [], []
    for d in range(3):
        lead_zero.append(spread(rows, 1 + d) * mass_x + spread(rows, 4 + 3 * d) * mass_slope)
        lead_one.append(spread(rows, 5 + 3 * d) * mass_x)
        lead_two.append(spread(rows, 6 + 3 * d) * mass_x)
    lead_zero, lead_one, lead_two = [
        jnp.concatenate([part.astype(BF16) for part in lead], axis=0)
        for lead in (lead_zero, lead_one, lead_two)
    ]
    first = contract(lead_zero, plane_zero)
    rest = contract(lead_one, plane_one) + contract(lead_two, plane_two)
    return first[:EDGE], first[EDGE:] + rest


def interpolate(rows, grid_rows):
    width = rows.shape[0] // FIELDS * LANES
    node = lax.broadcasted_iota(jnp.int32, (EDGE, width), 0).astype(F32)
    weight_x, slope_x = stencil(rows, node, 0)
    moment_zero, moment_one, moment_two = [
        jnp.dot(grid_rows, plane, preferred_element_type=F32) for plane in planes(rows, node)
    ]
    slope_x = 4.0 * slope_x
    weight_four = 4.0 * weight_x
    velocity, affine = [], []
    for d in range(3):
        part = slice(d * EDGE, (d + 1) * EDGE)

        def total(factor, moment):
            return jnp.sum(factor * moment[part], axis=0, keepdims=True)

        velocity.append(total(weight_x, moment_zero))
        affine.append(total(slope_x, moment_zero))
        affine.append(total(weight_four, moment_one))
        affine.append(total(weight_four, moment_two))
    return velocity + affine


def grid_kernel(
    tiles_ref, arrived_ref, drag_ref, grid_ref, out_ref, order_ref, sums_ref, round_ref, stage_ref
):
    slots = arrived_ref.shape[0]
    tile_count = drag_ref.shape[0]
    plane_size = EDGE * EDGE

    def collect(s, filled):
        order_ref[filled] = s
        return filled + (tiles_ref[s] >= 0).astype(jnp.int32)

    order_ref[0] = 0
    filled = lax.fori_loop(0, slots, collect, 0)
    last = order_ref[jnp.maximum(filled - 1, 0)]
    for u in range(UNROLL):
        order_ref[filled + u] = last

    def start(t, carry):
        for x in range(EDGE):
            sums_ref[t, x : x + 1, :] = drag_ref[
                pl.ds(t, 1), x * plane_size : (x + 1) * plane_size
            ]
        sums_ref[t, EDGE:, :] = jnp.zeros((3 * EDGE, plane_size), F32)
        return carry

    lax.fori_loop(0, tile_count, start, 0)
    steps = (filled + UNROLL - 1) // UNROLL

    def scatter(step, carry):
        results = []
        for u in range(UNROLL):
            at = step * UNROLL + u
            s = order_ref[at]
            results.append(
                (
                    jnp.where(at < filled, tiles_ref[s], tile_count),
                    deposit(arrived_ref[s].astype(F32)),
                )
            )
        for tile, (mass, momentum) in results:
            sums_ref[tile, :EDGE, :] += mass
            sums_ref[tile, EDGE:, :] += momentum
        return carry

    lax.fori_loop(0, steps, scatter, 0)

    def divide(t, carry):
        mass = sums_ref[t, :EDGE, :]
        parts = [
            sums_ref[t, (d + 1) * EDGE : (d + 2) * EDGE, :] / mass for d in range(3)
        ]
        velocity = jnp.concatenate(parts, axis=0)
        round_ref[t] = velocity.astype(BF16)
        for d in range(3):
            for x in range(EDGE):
                grid_ref[t, d : d + 1, x * plane_size : (x + 1) * plane_size] = parts[d][
                    x : x + 1
                ]
        return carry

    lax.fori_loop(0, tile_count, divide, 0)

    def gather(step, carry):
        for u in range(UNROLL):
            s = order_ref[step * UNROLL + u]
            results = interpolate(arrived_ref[s].astype(F32), round_ref[tiles_ref[s]])
            quarters = results[0].shape[1] // LANES
            for a in range(RESULTS):
                for q in range(quarters):
                    row = q * RESULTS + a
                    stage_ref[u, row : row + 1] = results[a][:, q * LANES : (q + 1) * LANES]
            out_ref[s] = stage_ref[u].astype(BF16)
        return carry

    lax.fori_loop(0, steps, gather, 0)


def grid_step(tiles, arrived, drag):
    slots, rows, _ = arrived.shape
    out_rows = rows // FIELDS * RESULTS
    tile_count, cells = drag.shape
    plane_size = EDGE * EDGE
    smem = pl.BlockSpec(memory_space=pltpu.SMEM)
    vmem = pl.BlockSpec(memory_space=pltpu.VMEM)
    return pl.pallas_call(
        grid_kernel,
        name="grid_step",
        out_shape=(
            jax.ShapeDtypeStruct((tile_count, 3, cells), F32),
            jax.ShapeDtypeStruct((slots, out_rows, LANES), BF16),
        ),
        in_specs=[smem, vmem, vmem],
        out_specs=(vmem, vmem),
        scratch_shapes=[
            pltpu.SMEM((slots + UNROLL,), jnp.int32),
            pltpu.VMEM((tile_count + 1, 4 * EDGE, plane_size), F32),
            pltpu.VMEM((tile_count, 3 * EDGE, plane_size), BF16),
            pltpu.VMEM((UNROLL, out_rows, LANES), F32),
        ],
        compiler_params=pltpu.CompilerParams(vmem_limit_bytes=48 << 20),
    )(tiles, arrived, drag)


def unpack_kernel(dest_ref, count_ref, returned_ref, velocity_ref, affine_ref):
    blocks = dest_ref.shape[0]
    width = velocity_ref.shape[1] // blocks
    lane = lax.broadcasted_iota(jnp.int32, (1, LANES), 1)

    def unpack(block, carry):
        rows = returned_ref[dest_ref[block]].astype(F32)
        for q in range(width // LANES):
            present = lane + q * LANES < count_ref[block]
            cols = pl.ds(pl.multiple_of(block * width + q * LANES, LANES), LANES)
            part = jnp.where(present, rows[q * RESULTS : (q + 1) * RESULTS], 0.0)
            velocity_ref[:, cols] = part[:3]
            affine_ref[:, cols] = part[3:]
        return carry

    lax.fori_loop(0, blocks, unpack, 0)


def unpack(dest, count, returned, width):
    particles = dest.shape[0] * width
    smem = pl.BlockSpec(memory_space=pltpu.SMEM)
    vmem = pl.BlockSpec(memory_space=pltpu.VMEM)
    return pl.pallas_call(
        unpack_kernel,
        name="unpack",
        out_shape=(
            jax.ShapeDtypeStruct((3, particles), F32),
            jax.ShapeDtypeStruct((9, particles), F32),
        ),
        in_specs=[smem, smem, vmem],
        out_specs=(vmem, vmem),
        compiler_params=pltpu.CompilerParams(vmem_limit_bytes=48 << 20),
    )(dest, count, returned)


def exchange(value):
    return lax.all_to_all(value, GROUP_AXES, split_axis=0, concat_axis=0, tiled=True)


def per_device(
    particle_mass,
    particle_velocity,
    particle_affine,
    particle_cell,
    particle_fraction,
    block_owner,
    block_slot,
    block_count,
    cell_drag,
):
    group_size = lax.axis_size(GROUP_AXES)
    blocks = block_count.shape[0]
    capacity = max(1, 2 * blocks // group_size)
    slots = group_size * capacity
    payload, tiles, dest = pack(
        capacity,
        slots,
        group_size,
        block_owner[:, 0],
        block_slot,
        block_count,
        particle_mass,
        particle_velocity,
        particle_affine,
        particle_cell,
        particle_fraction,
    )
    arrived_tiles = exchange(tiles)
    arrived = exchange(payload)
    grid_velocity, results = grid_step(arrived_tiles, arrived, cell_drag)
    returned = exchange(results)
    new_velocity, new_affine = unpack(
        dest, block_count, returned, particle_mass.shape[0] // blocks
    )
    return grid_velocity, new_velocity, new_affine


def solution(mesh):
    everywhere = ("gx", "gy", "gz")
    return jax.shard_map(
        per_device,
        mesh=mesh,
        in_specs=(
            P(everywhere),
            P(None, everywhere),
            P(None, everywhere),
            P(None, everywhere),
            P(None, everywhere),
            P(everywhere, None),
            P(everywhere),
            P(everywhere),
            P(everywhere, None),
        ),
        out_specs=(P(everywhere, None, None), P(None, everywhere), P(None, everywhere)),
        check_vma=False,
    )
```

```python
import functools

import jax
import jax.numpy as jnp
from jax import lax
from jax.experimental import pallas as pl
from jax.experimental.pallas import tpu as pltpu
from jax.sharding import PartitionSpec as P

EDGE = 16
QUANT = 1024
LANES = 128
FIELDS = 20
RESULTS = 12
UNROLL = 4
HALVES = 2
GROUP_AXES = ("gy", "gz")
F32 = jnp.float32
BF16 = jnp.bfloat16


SMEM = pl.BlockSpec(memory_space=pltpu.SMEM)
VMEM = pl.BlockSpec(memory_space=pltpu.VMEM)
PARAMS = pltpu.CompilerParams(vmem_limit_bytes=48 << 20)


def cost(flops):
    return pl.CostEstimate(flops=flops, bytes_accessed=1 << 22, transcendentals=0)


def pack_kernel(
    portion,
    owner_ref,
    slot_ref,
    count_ref,
    mass_ref,
    velocity_ref,
    affine_ref,
    cell_ref,
    fraction_ref,
    *rest,
):
    payload_refs, (dest_ref, used_ref, stage_ref) = rest[:-3], rest[-3:]
    blocks = owner_ref.shape[0]
    group_size = used_ref.shape[0]
    width = mass_ref.shape[1]
    half_rows = payload_refs[0].shape[1]
    half_width = width // HALVES

    def clear_used(i, carry):
        used_ref[i] = 0
        return carry

    lax.fori_loop(0, group_size, clear_used, 0)
    lane = lax.broadcasted_iota(jnp.int32, (1, width), 1)

    def clear_marks(i, carry):
        for payload_ref in payload_refs:
            payload_ref[i, 16:32, :] = jnp.full((16, LANES), -1.0, BF16)
        return carry

    lax.fori_loop(0, payload_refs[0].shape[0], clear_marks, 0)

    def pack(block, carry):
        owner = owner_ref[block]
        rank = used_ref[owner]
        used_ref[owner] = rank + 1
        chunk = rank // portion
        where = owner * portion + rank % portion
        dest_ref[block] = chunk * (group_size * portion) + where
        count = count_ref[block]
        mark = slot_ref[block].astype(F32)
        cols = pl.ds(pl.multiple_of(block * width, LANES), width)
        live = jnp.where(lane < count, mass_ref[pl.ds(block, 1), :], 0.0)
        velocity = velocity_ref[:, cols]
        affine = affine_ref[:, cols]
        code = cell_ref[:, cols] * QUANT + fraction_ref[:, cols]
        high = (code >> 7).astype(F32)
        low = (code & 127).astype(F32)
        for q in range(width // LANES):
            part = slice(q * LANES, (q + 1) * LANES)
            first_lane = q * LANES // half_width * half_width
            base = q * FIELDS
            stage_ref[base : base + 1] = live[:, part]
            stage_ref[base + 1 : base + 4] = velocity[:, part]
            stage_ref[base + 4 : base + 13] = affine[:, part]
            stage_ref[base + 13 : base + 16] = high[:, part]
            stage_ref[base + 16 : base + 19] = low[:, part]
            stage_ref[base + 19 : base + 20] = jnp.full(
                (1, LANES), jnp.where(count > first_lane, mark, -1.0), F32
            )
        for c, payload_ref in enumerate(payload_refs):

            @pl.when(chunk == c)
            def _():
                for h in range(HALVES):
                    payload_ref[where * HALVES + h] = stage_ref[
                        h * half_rows : (h + 1) * half_rows
                    ].astype(BF16)

        return carry

    lax.fori_loop(0, blocks, pack, 0)


def pack(chunks, portion, group_size, owner, slot, count, mass, velocity, affine, cell, fraction):
    blocks = owner.shape[0]
    width = mass.shape[0] // blocks
    rows = width // LANES * FIELDS
    payload = jax.ShapeDtypeStruct(
        (group_size * portion * HALVES, rows // HALVES, LANES), BF16
    )
    outs = pl.pallas_call(
        functools.partial(pack_kernel, portion),
        name="pack",
        out_shape=(payload,) * chunks + (jax.ShapeDtypeStruct((blocks,), jnp.int32),),
        in_specs=[SMEM] * 3 + [VMEM] * 5,
        out_specs=(VMEM,) * chunks + (SMEM,),
        scratch_shapes=[pltpu.SMEM((group_size,), jnp.int32), pltpu.VMEM((rows, LANES), F32)],
        compiler_params=PARAMS,
    )(owner, slot, count, mass.reshape(blocks, width), velocity, affine, cell, fraction)
    return outs[:-1], outs[-1]


def twice(rows):
    return jnp.concatenate([rows, rows], axis=0)


def load_item(u, item_ref, fields_ref):
    rows = item_ref.shape[0]
    quarters = rows // FIELDS
    first = u * rows
    fields_ref[first : first + rows] = item_ref[...].astype(F32)
    for q in range(quarters):
        base = first + q * FIELDS
        fields_ref[base + 13 : base + 16] = (
            fields_ref[base + 13 : base + 16] * (128.0 / QUANT)
            + fields_ref[base + 16 : base + 19] * (1.0 / QUANT)
            + (0.5 + 0.5 / QUANT)
        )

    def spread(field):
        return twice(
            jnp.concatenate(
                [
                    fields_ref[pl.ds(first + q * FIELDS + field, 8, stride=0), :]
                    for q in range(quarters)
                ],
                axis=1,
            )
        )

    return spread, quarters


def stencil(spread, node, dim):
    offset = node - spread(13 + dim)
    magnitude = jnp.abs(offset)
    outer_part = jnp.maximum(1.5 - magnitude, 0.0)
    weight = jnp.where(
        magnitude < 0.5, 0.75 - magnitude * magnitude, 0.5 * outer_part * outer_part
    )
    return weight, weight * offset


def planes(u, spread, quarters, node, rows_ref):
    factors_y = stencil(spread, node, 1)
    factors_z = [factor.astype(BF16) for factor in stencil(spread, node, 2)]
    firsts = [(u * 2 + k) * quarters * EDGE for k in range(2)]
    for first, factor in zip(firsts, factors_y):
        for q in range(quarters):
            rows_ref[first + q * EDGE : first + (q + 1) * EDGE] = factor[
                :, q * LANES : (q + 1) * LANES
            ]

    def row(first, y):
        return jnp.concatenate(
            [
                twice(rows_ref[pl.ds(first + q * EDGE + y, 8, stride=0), :]).astype(BF16)
                for q in range(quarters)
            ],
            axis=1,
        )

    zero, one, two = [], [], []
    for y in range(EDGE):
        weight_row, slope_row = row(firsts[0], y), row(firsts[1], y)
        zero.append(weight_row * factors_z[0])
        one.append(slope_row * factors_z[0])
        two.append(weight_row * factors_z[1])
    return [jnp.concatenate(parts, axis=0) for parts in (zero, one, two)]


def nodes(quarters):
    return lax.broadcasted_iota(jnp.int32, (EDGE, quarters * LANES), 0).astype(F32)


def deposit(u, item_ref, fields_ref, rows_ref):
    spread, quarters = load_item(u, item_ref, fields_ref)
    node = nodes(quarters)
    weight_x, slope_x = stencil(spread, node, 0)
    mass = spread(0)
    mass_x = mass * weight_x
    mass_slope = mass * slope_x
    nothing = jnp.zeros(mass_x.shape, BF16)
    lead_zero, lead_one, lead_two = [mass_x.astype(BF16)], [nothing], [nothing]
    for d in range(3):
        lead_zero.append(
            (spread(1 + d) * mass_x + spread(4 + 3 * d) * mass_slope).astype(BF16)
        )
        lead_one.append((spread(5 + 3 * d) * mass_x).astype(BF16))
        lead_two.append((spread(6 + 3 * d) * mass_x).astype(BF16))
    lead = jnp.concatenate(
        [jnp.concatenate(part, axis=0) for part in (lead_zero, lead_one, lead_two)], axis=1
    )
    plane = jnp.concatenate(planes(u, spread, quarters, node, rows_ref), axis=1)
    return lax.dot_general(lead, plane, (((1,), (1,)), ((), ())), preferred_element_type=F32)


def interpolate(u, item_ref, grid_rows, fields_ref, rows_ref, parts_ref):
    spread, quarters = load_item(u, item_ref, fields_ref)
    node = nodes(quarters)
    weight_x, slope_x = stencil(spread, node, 0)
    moments = [
        jnp.dot(grid_rows, plane, preferred_element_type=F32)
        for plane in planes(u, spread, quarters, node, rows_ref)
    ]
    slope_four = 4.0 * slope_x
    weight_four = 4.0 * weight_x
    first = u * quarters * RESULTS * 8
    for d in range(3):
        span = slice(d * EDGE, (d + 1) * EDGE)
        entries = (
            (d, weight_x, moments[0]),
            (3 + 3 * d, slope_four, moments[0]),
            (4 + 3 * d, weight_four, moments[1]),
            (5 + 3 * d, weight_four, moments[2]),
        )
        for entry, factor, moment in entries:
            product = factor * moment[span]
            partial = product[:8] + product[8:]
            for q in range(quarters):
                at = first + (q * RESULTS + entry) * 8
                parts_ref[at : at + 8] = partial[:, q * LANES : (q + 1) * LANES]
    groups = []
    for g in range(quarters * RESULTS // 8):
        total = parts_ref[pl.ds(first + g * 64, 8, stride=8), :]
        for j in range(1, 8):
            total = total + parts_ref[pl.ds(first + g * 64 + j, 8, stride=8), :]
        groups.append(total)
    return jnp.concatenate(groups, axis=0).astype(BF16)


def collect_filled(tiles_ref, order_ref):
    def collect(s, filled):
        order_ref[filled] = s
        return filled + (tiles_ref[s] >= 0).astype(jnp.int32)

    order_ref[0] = 0
    filled = lax.fori_loop(0, tiles_ref.shape[0], collect, 0)
    last = order_ref[jnp.maximum(filled - 1, 0)]
    for u in range(UNROLL):
        order_ref[filled + u] = last
    return filled


def scatter_items(tiles_ref, arrived_ref, sums_ref, order_ref, fields_ref, rows_ref):
    filled = collect_filled(tiles_ref, order_ref)
    spare = sums_ref.shape[0] - 1

    def scatter(step, carry):
        results = []
        for u in range(UNROLL):
            at = step * UNROLL + u
            s = order_ref[at]
            tile = jnp.where(at < filled, tiles_ref[s], spare)
            results.append((tile, deposit(u, arrived_ref.at[s], fields_ref, rows_ref)))
        for tile, sums in results:
            sums_ref[tile] += sums
        return carry

    lax.fori_loop(0, (filled + UNROLL - 1) // UNROLL, scatter, 0)


def gather_items(
    tiles_ref, arrived_ref, round_ref, out_ref, order_ref, fields_ref, rows_ref, parts_ref
):
    filled = collect_filled(tiles_ref, order_ref)

    def gather(step, carry):
        for u in range(UNROLL):
            s = order_ref[step * UNROLL + u]
            out_ref[s] = interpolate(
                u,
                arrived_ref.at[s],
                round_ref[jnp.maximum(tiles_ref[s], 0)],
                fields_ref,
                rows_ref,
                parts_ref,
            )
        return carry

    lax.fori_loop(0, (filled + UNROLL - 1) // UNROLL, gather, 0)


def work_shapes(slots, item_rows):
    quarters = item_rows // FIELDS
    return [
        pltpu.SMEM((slots + UNROLL,), jnp.int32),
        pltpu.VMEM((UNROLL * item_rows, LANES), F32),
        pltpu.VMEM((UNROLL * 2 * quarters * EDGE, LANES), F32),
        pltpu.VMEM((UNROLL * quarters * RESULTS * 8, LANES), F32),
    ]


def start_kernel(drag_ref, sums_ref):
    plane_size = EDGE * EDGE

    def start(t, carry):
        for x in range(EDGE):
            sums_ref[t, x : x + 1, :] = drag_ref[
                pl.ds(t, 1), x * plane_size : (x + 1) * plane_size
            ]
        sums_ref[t, EDGE:, :] = jnp.zeros((3 * EDGE, plane_size), F32)
        return carry

    lax.fori_loop(0, drag_ref.shape[0], start, 0)
    sums_ref[drag_ref.shape[0]] = jnp.zeros((4 * EDGE, plane_size), F32)


def start_sums(drag):
    return pl.pallas_call(
        start_kernel,
        name="start_sums",
        out_shape=jax.ShapeDtypeStruct((drag.shape[0] + 1, 4 * EDGE, EDGE * EDGE), F32),
        in_specs=[VMEM],
        out_specs=VMEM,
        compiler_params=PARAMS,
        cost_estimate=cost(1 << 20),
    )(drag)


def copy_sums(before_ref, sums_ref):
    def copy(t, carry):
        sums_ref[t] = before_ref[t]
        return carry

    lax.fori_loop(0, sums_ref.shape[0], copy, 0)


def scatter_kernel(
    tiles_ref, arrived_ref, before_ref, sums_ref, order_ref, fields_ref, rows_ref, parts_ref
):
    copy_sums(before_ref, sums_ref)
    scatter_items(tiles_ref, arrived_ref, sums_ref, order_ref, fields_ref, rows_ref)


def scatter_step(tiles, arrived, sums):
    return pl.pallas_call(
        scatter_kernel,
        name="scatter_step",
        out_shape=jax.ShapeDtypeStruct(sums.shape, F32),
        in_specs=[SMEM, VMEM, VMEM],
        out_specs=VMEM,
        scratch_shapes=work_shapes(arrived.shape[0], arrived.shape[1]),
        compiler_params=PARAMS,
        cost_estimate=cost(10**10),
    )(tiles, arrived, sums)


def grid_kernel(
    last_tiles_ref,
    last_ref,
    tiles_ref,
    arrived_ref,
    before_ref,
    grid_ref,
    round_ref,
    out_ref,
    order_ref,
    fields_ref,
    rows_ref,
    parts_ref,
    sums_ref,
):
    plane_size = EDGE * EDGE
    copy_sums(before_ref, sums_ref)
    scatter_items(last_tiles_ref, last_ref, sums_ref, order_ref, fields_ref, rows_ref)

    def divide(t, carry):
        mass = sums_ref[t, :EDGE, :]
        parts = [sums_ref[t, (d + 1) * EDGE : (d + 2) * EDGE, :] / mass for d in range(3)]
        round_ref[t] = jnp.concatenate(parts, axis=0).astype(BF16)
        for d in range(3):
            for x in range(EDGE):
                grid_ref[t, d : d + 1, x * plane_size : (x + 1) * plane_size] = parts[d][
                    x : x + 1
                ]
        return carry

    lax.fori_loop(0, round_ref.shape[0], divide, 0)
    gather_items(
        tiles_ref, arrived_ref, round_ref, out_ref, order_ref, fields_ref, rows_ref, parts_ref
    )


def result_shape(arrived):
    slots, rows, _ = arrived.shape
    return jax.ShapeDtypeStruct((slots, rows // FIELDS * RESULTS, LANES), BF16)


def grid_step(last_tiles, last, tiles, arrived, sums):
    tile_count = sums.shape[0] - 1
    plane_size = EDGE * EDGE
    return pl.pallas_call(
        grid_kernel,
        name="grid_step",
        out_shape=(
            jax.ShapeDtypeStruct((tile_count, 3, EDGE * plane_size), F32),
            jax.ShapeDtypeStruct((tile_count, 3 * EDGE, plane_size), BF16),
            result_shape(arrived),
        ),
        in_specs=[SMEM, VMEM, SMEM, VMEM, VMEM],
        out_specs=(VMEM,) * 3,
        scratch_shapes=work_shapes(arrived.shape[0], arrived.shape[1])
        + [pltpu.VMEM(sums.shape, F32)],
        compiler_params=PARAMS,
        cost_estimate=cost(10**10),
    )(last_tiles, last, tiles, arrived, sums)


def gather_step(tiles, arrived, rounded):
    return pl.pallas_call(
        gather_items,
        name="gather_step",
        out_shape=result_shape(arrived),
        in_specs=[SMEM, VMEM, VMEM],
        out_specs=VMEM,
        scratch_shapes=work_shapes(arrived.shape[0], arrived.shape[1]),
        compiler_params=PARAMS,
        cost_estimate=cost(10**10),
    )(tiles, arrived, rounded)


def unpack_kernel(dest_ref, count_ref, *refs):
    returned_refs, (velocity_ref, affine_ref) = refs[:-2], refs[-2:]
    blocks = dest_ref.shape[0]
    width = velocity_ref.shape[1] // blocks
    slots = returned_refs[0].shape[0] // HALVES
    half_width = width // HALVES
    lane = lax.broadcasted_iota(jnp.int32, (1, LANES), 1)

    def unpack(block, carry):
        dest = dest_ref[block]
        count = count_ref[block]
        for c, returned_ref in enumerate(returned_refs):

            @pl.when(dest // slots == c)
            def _():
                for h in range(HALVES):
                    rows = returned_ref[(dest - c * slots) * HALVES + h].astype(F32)
                    for q in range(half_width // LANES):
                        first = h * half_width + q * LANES
                        cols = pl.ds(pl.multiple_of(block * width + first, LANES), LANES)
                        part = jnp.where(
                            lane + first < count, rows[q * RESULTS : (q + 1) * RESULTS], 0.0
                        )
                        velocity_ref[:, cols] = part[:3]
                        affine_ref[:, cols] = part[3:]

        return carry

    lax.fori_loop(0, blocks, unpack, 0)


def unpack(dest, count, returned, width):
    particles = dest.shape[0] * width
    return pl.pallas_call(
        unpack_kernel,
        name="unpack",
        out_shape=(
            jax.ShapeDtypeStruct((3, particles), F32),
            jax.ShapeDtypeStruct((9, particles), F32),
        ),
        in_specs=[SMEM, SMEM] + [VMEM] * len(returned),
        out_specs=(VMEM, VMEM),
        compiler_params=PARAMS,
    )(dest, count, *returned)


def tile_marks(arrived):
    return arrived[:, FIELDS - 1, 0].astype(jnp.int32)


def exchange(value):
    return lax.all_to_all(value, GROUP_AXES, split_axis=0, concat_axis=0, tiled=True)


def per_device(
    particle_mass,
    particle_velocity,
    particle_affine,
    particle_cell,
    particle_fraction,
    block_owner,
    block_slot,
    block_count,
    cell_drag,
):
    group_size = lax.axis_size(GROUP_AXES)
    blocks = block_count.shape[0]
    capacity = max(1, 2 * blocks // group_size)
    chunks = 2 if capacity % 2 == 0 else 1
    portion = capacity // chunks
    payloads, dest = pack(
        chunks,
        portion,
        group_size,
        block_owner[:, 0],
        block_slot,
        block_count,
        particle_mass,
        particle_velocity,
        particle_affine,
        particle_cell,
        particle_fraction,
    )
    arrived = [exchange(payload) for payload in payloads]
    tiles = [tile_marks(part) for part in arrived]
    sums = start_sums(cell_drag)
    for c in range(chunks - 1):
        sums = scatter_step(tiles[c], arrived[c], sums)
    grid_velocity, rounded, results = grid_step(
        tiles[-1], arrived[-1], tiles[0], arrived[0], sums
    )
    returned = [exchange(results)]
    for c in range(1, chunks):
        returned.append(exchange(gather_step(tiles[c], arrived[c], rounded)))
    new_velocity, new_affine = unpack(
        dest, block_count, returned, particle_mass.shape[0] // blocks
    )
    return grid_velocity, new_velocity, new_affine


def solution(mesh):
    everywhere = ("gx", "gy", "gz")
    return jax.shard_map(
        per_device,
        mesh=mesh,
        in_specs=(
            P(everywhere),
            P(None, everywhere),
            P(None, everywhere),
            P(None, everywhere),
            P(None, everywhere),
            P(everywhere, None),
            P(everywhere),
            P(everywhere),
            P(everywhere, None),
        ),
        out_specs=(P(everywhere, None, None), P(None, everywhere), P(None, everywhere)),
        check_vma=False,
    )
```

```python
import functools

import jax
import jax.numpy as jnp
from jax import lax
from jax.experimental import pallas as pl
from jax.experimental.pallas import tpu as pltpu
from jax.sharding import PartitionSpec as P

EDGE = 16
QUANT = 1024
LANES = 128
FIELDS = 20
RESULTS = 12
UNROLL = 4
HALVES = 2
GROUP_AXES = ("gy", "gz")
F32 = jnp.float32
BF16 = jnp.bfloat16


SMEM = pl.BlockSpec(memory_space=pltpu.SMEM)
VMEM = pl.BlockSpec(memory_space=pltpu.VMEM)
PARAMS = pltpu.CompilerParams(vmem_limit_bytes=20 << 20)


def cost(flops):
    return pl.CostEstimate(flops=flops, bytes_accessed=1 << 22, transcendentals=0)


def pack_kernel(
    portion,
    owner_ref,
    slot_ref,
    count_ref,
    mass_ref,
    velocity_ref,
    affine_ref,
    cell_ref,
    fraction_ref,
    *rest,
):
    payload_refs, (dest_ref, used_ref, stage_ref) = rest[:-3], rest[-3:]
    blocks = owner_ref.shape[0]
    group_size = used_ref.shape[0]
    width = mass_ref.shape[1]
    half_rows = payload_refs[0].shape[1]
    half_width = width // HALVES

    def clear_used(i, carry):
        used_ref[i] = 0
        return carry

    lax.fori_loop(0, group_size, clear_used, 0)
    lane = lax.broadcasted_iota(jnp.int32, (1, width), 1)

    def clear_marks(i, carry):
        for payload_ref in payload_refs:
            payload_ref[i, 16:32, :] = jnp.full((16, LANES), -1.0, BF16)
        return carry

    lax.fori_loop(0, payload_refs[0].shape[0], clear_marks, 0)

    def pack(block, carry):
        owner = owner_ref[block]
        rank = used_ref[owner]
        used_ref[owner] = rank + 1
        chunk = rank // portion
        where = owner * portion + rank % portion
        dest_ref[block] = chunk * (group_size * portion) + where
        count = count_ref[block]
        mark = slot_ref[block].astype(F32)
        cols = pl.ds(pl.multiple_of(block * width, LANES), width)
        live = jnp.where(lane < count, mass_ref[pl.ds(block, 1), :], 0.0)
        velocity = velocity_ref[:, cols]
        affine = affine_ref[:, cols]
        code = cell_ref[:, cols] * QUANT + fraction_ref[:, cols]
        high = (code >> 7).astype(F32)
        low = (code & 127).astype(F32)
        for q in range(width // LANES):
            part = slice(q * LANES, (q + 1) * LANES)
            first_lane = q * LANES // half_width * half_width
            base = q * FIELDS
            stage_ref[base : base + 1] = live[:, part]
            stage_ref[base + 1 : base + 4] = velocity[:, part]
            stage_ref[base + 4 : base + 13] = affine[:, part]
            stage_ref[base + 13 : base + 16] = high[:, part]
            stage_ref[base + 16 : base + 19] = low[:, part]
            stage_ref[base + 19 : base + 20] = jnp.full(
                (1, LANES), jnp.where(count > first_lane, mark, -1.0), F32
            )
        for c, payload_ref in enumerate(payload_refs):

            @pl.when(chunk == c)
            def _():
                for h in range(HALVES):
                    payload_ref[where * HALVES + h] = stage_ref[
                        h * half_rows : (h + 1) * half_rows
                    ].astype(BF16)

        return carry

    lax.fori_loop(0, blocks, pack, 0)


def pack(chunks, portion, group_size, owner, slot, count, mass, velocity, affine, cell, fraction):
    blocks = owner.shape[0]
    width = mass.shape[0] // blocks
    rows = width // LANES * FIELDS
    payload = jax.ShapeDtypeStruct(
        (group_size * portion * HALVES, rows // HALVES, LANES), BF16
    )
    outs = pl.pallas_call(
        functools.partial(pack_kernel, portion),
        name="pack",
        out_shape=(payload,) * chunks + (jax.ShapeDtypeStruct((blocks,), jnp.int32),),
        in_specs=[SMEM] * 3 + [VMEM] * 5,
        out_specs=(VMEM,) * chunks + (SMEM,),
        scratch_shapes=[pltpu.SMEM((group_size,), jnp.int32), pltpu.VMEM((rows, LANES), F32)],
        compiler_params=PARAMS,
    )(owner, slot, count, mass.reshape(blocks, width), velocity, affine, cell, fraction)
    return outs[:-1], outs[-1]


def twice(rows):
    return jnp.concatenate([rows, rows], axis=0)


def load_item(u, item_ref, fields_ref):
    rows = item_ref.shape[0]
    quarters = rows // FIELDS
    first = u * rows
    fields_ref[first : first + rows] = item_ref[...].astype(F32)
    for q in range(quarters):
        base = first + q * FIELDS
        fields_ref[base + 13 : base + 16] = (
            fields_ref[base + 13 : base + 16] * (128.0 / QUANT)
            + fields_ref[base + 16 : base + 19] * (1.0 / QUANT)
            + (0.5 + 0.5 / QUANT)
        )

    def spread(field):
        return twice(
            jnp.concatenate(
                [
                    fields_ref[pl.ds(first + q * FIELDS + field, 8, stride=0), :]
                    for q in range(quarters)
                ],
                axis=1,
            )
        )

    return spread, quarters


def stencil(spread, node, dim):
    offset = node - spread(13 + dim)
    magnitude = jnp.abs(offset)
    outer_part = jnp.maximum(1.5 - magnitude, 0.0)
    weight = jnp.where(
        magnitude < 0.5, 0.75 - magnitude * magnitude, 0.5 * outer_part * outer_part
    )
    return weight, weight * offset


def planes(u, spread, quarters, node, rows_ref):
    factors_y = stencil(spread, node, 1)
    factors_z = [factor.astype(BF16) for factor in stencil(spread, node, 2)]
    firsts = [(u * 2 + k) * quarters * EDGE for k in range(2)]
    for first, factor in zip(firsts, factors_y):
        for q in range(quarters):
            rows_ref[first + q * EDGE : first + (q + 1) * EDGE] = factor[
                :, q * LANES : (q + 1) * LANES
            ]

    def row(first, y):
        return jnp.concatenate(
            [
                twice(rows_ref[pl.ds(first + q * EDGE + y, 8, stride=0), :]).astype(BF16)
                for q in range(quarters)
            ],
            axis=1,
        )

    zero, one, two = [], [], []
    for y in range(EDGE):
        weight_row, slope_row = row(firsts[0], y), row(firsts[1], y)
        zero.append(weight_row * factors_z[0])
        one.append(slope_row * factors_z[0])
        two.append(weight_row * factors_z[1])
    return [jnp.concatenate(parts, axis=0) for parts in (zero, one, two)]


def nodes(quarters):
    return lax.broadcasted_iota(jnp.int32, (EDGE, quarters * LANES), 0).astype(F32)


def deposit(u, item_ref, fields_ref, rows_ref):
    spread, quarters = load_item(u, item_ref, fields_ref)
    node = nodes(quarters)
    weight_x, slope_x = stencil(spread, node, 0)
    mass = spread(0)
    mass_x = mass * weight_x
    mass_slope = mass * slope_x
    nothing = jnp.zeros(mass_x.shape, BF16)
    lead_zero, lead_one, lead_two = [mass_x.astype(BF16)], [nothing], [nothing]
    for d in range(3):
        lead_zero.append(
            (spread(1 + d) * mass_x + spread(4 + 3 * d) * mass_slope).astype(BF16)
        )
        lead_one.append((spread(5 + 3 * d) * mass_x).astype(BF16))
        lead_two.append((spread(6 + 3 * d) * mass_x).astype(BF16))
    lead = jnp.concatenate(
        [jnp.concatenate(part, axis=0) for part in (lead_zero, lead_one, lead_two)], axis=1
    )
    plane = jnp.concatenate(planes(u, spread, quarters, node, rows_ref), axis=1)
    return lax.dot_general(lead, plane, (((1,), (1,)), ((), ())), preferred_element_type=F32)


def interpolate(u, item_ref, grid_rows, fields_ref, rows_ref, parts_ref):
    spread, quarters = load_item(u, item_ref, fields_ref)
    node = nodes(quarters)
    weight_x, slope_x = stencil(spread, node, 0)
    moments = [
        jnp.dot(grid_rows, plane, preferred_element_type=F32)
        for plane in planes(u, spread, quarters, node, rows_ref)
    ]
    slope_four = 4.0 * slope_x
    weight_four = 4.0 * weight_x
    first = u * quarters * RESULTS * 8
    for d in range(3):
        span = slice(d * EDGE, (d + 1) * EDGE)
        entries = (
            (d, weight_x, moments[0]),
            (3 + 3 * d, slope_four, moments[0]),
            (4 + 3 * d, weight_four, moments[1]),
            (5 + 3 * d, weight_four, moments[2]),
        )
        for entry, factor, moment in entries:
            product = factor * moment[span]
            partial = product[:8] + product[8:]
            for q in range(quarters):
                at = first + (q * RESULTS + entry) * 8
                parts_ref[at : at + 8] = partial[:, q * LANES : (q + 1) * LANES]
    groups = []
    for g in range(quarters * RESULTS // 8):
        total = parts_ref[pl.ds(first + g * 64, 8, stride=8), :]
        for j in range(1, 8):
            total = total + parts_ref[pl.ds(first + g * 64 + j, 8, stride=8), :]
        groups.append(total)
    return jnp.concatenate(groups, axis=0).astype(BF16)


def collect_filled(tiles_ref, order_ref):
    def collect(s, filled):
        order_ref[filled] = s
        return filled + (tiles_ref[s] >= 0).astype(jnp.int32)

    order_ref[0] = 0
    filled = lax.fori_loop(0, tiles_ref.shape[0], collect, 0)
    last = order_ref[jnp.maximum(filled - 1, 0)]
    for u in range(UNROLL):
        order_ref[filled + u] = last
    return filled


def scatter_items(tiles_ref, arrived_ref, sums_ref, order_ref, fields_ref, rows_ref):
    filled = collect_filled(tiles_ref, order_ref)
    spare = sums_ref.shape[0] - 1

    def scatter(step, carry):
        results = []
        for u in range(UNROLL):
            at = step * UNROLL + u
            s = order_ref[at]
            tile = jnp.where(at < filled, tiles_ref[s], spare)
            results.append((tile, deposit(u, arrived_ref.at[s], fields_ref, rows_ref)))
        for tile, sums in results:
            sums_ref[tile] += sums
        return carry

    lax.fori_loop(0, (filled + UNROLL - 1) // UNROLL, scatter, 0)


def gather_items(
    tiles_ref, arrived_ref, round_ref, out_ref, order_ref, fields_ref, rows_ref, parts_ref
):
    filled = collect_filled(tiles_ref, order_ref)

    def gather(step, carry):
        for u in range(UNROLL):
            s = order_ref[step * UNROLL + u]
            out_ref[s] = interpolate(
                u,
                arrived_ref.at[s],
                round_ref[jnp.maximum(tiles_ref[s], 0)],
                fields_ref,
                rows_ref,
                parts_ref,
            )
        return carry

    lax.fori_loop(0, (filled + UNROLL - 1) // UNROLL, gather, 0)


def work_shapes(slots, item_rows):
    quarters = item_rows // FIELDS
    return [
        pltpu.SMEM((slots + UNROLL,), jnp.int32),
        pltpu.VMEM((UNROLL * item_rows, LANES), F32),
        pltpu.VMEM((UNROLL * 2 * quarters * EDGE, LANES), F32),
        pltpu.VMEM((UNROLL * quarters * RESULTS * 8, LANES), F32),
    ]


def start_kernel(drag_ref, sums_ref):
    plane_size = EDGE * EDGE

    def start(t, carry):
        for x in range(EDGE):
            sums_ref[t, x : x + 1, :] = drag_ref[
                pl.ds(t, 1), x * plane_size : (x + 1) * plane_size
            ]
        sums_ref[t, EDGE:, :] = jnp.zeros((3 * EDGE, plane_size), F32)
        return carry

    lax.fori_loop(0, drag_ref.shape[0], start, 0)
    sums_ref[drag_ref.shape[0]] = jnp.zeros((4 * EDGE, plane_size), F32)


def start_sums(drag):
    return pl.pallas_call(
        start_kernel,
        name="start_sums",
        out_shape=jax.ShapeDtypeStruct((drag.shape[0] + 1, 4 * EDGE, EDGE * EDGE), F32),
        in_specs=[VMEM],
        out_specs=VMEM,
        compiler_params=PARAMS,
        cost_estimate=cost(1 << 20),
    )(drag)


def copy_sums(before_ref, sums_ref):
    def copy(t, carry):
        sums_ref[t] = before_ref[t]
        return carry

    lax.fori_loop(0, sums_ref.shape[0], copy, 0)


def scatter_kernel(
    tiles_ref, arrived_ref, before_ref, sums_ref, order_ref, fields_ref, rows_ref, parts_ref
):
    copy_sums(before_ref, sums_ref)
    scatter_items(tiles_ref, arrived_ref, sums_ref, order_ref, fields_ref, rows_ref)


def scatter_step(tiles, arrived, sums):
    return pl.pallas_call(
        scatter_kernel,
        name="scatter_step",
        out_shape=jax.ShapeDtypeStruct(sums.shape, F32),
        in_specs=[SMEM, VMEM, VMEM],
        out_specs=VMEM,
        scratch_shapes=work_shapes(arrived.shape[0], arrived.shape[1]),
        compiler_params=PARAMS,
        cost_estimate=cost(10**10),
    )(tiles, arrived, sums)


def grid_kernel(
    last_tiles_ref,
    last_ref,
    tiles_ref,
    arrived_ref,
    before_ref,
    grid_ref,
    round_ref,
    out_ref,
    order_ref,
    fields_ref,
    rows_ref,
    parts_ref,
    sums_ref,
):
    plane_size = EDGE * EDGE
    copy_sums(before_ref, sums_ref)
    scatter_items(last_tiles_ref, last_ref, sums_ref, order_ref, fields_ref, rows_ref)

    def divide(t, carry):
        mass = sums_ref[t, :EDGE, :]
        parts = [sums_ref[t, (d + 1) * EDGE : (d + 2) * EDGE, :] / mass for d in range(3)]
        round_ref[t] = jnp.concatenate(parts, axis=0).astype(BF16)
        for d in range(3):
            for x in range(EDGE):
                grid_ref[d, pl.ds(t, 1), x * plane_size : (x + 1) * plane_size] = parts[d][
                    x : x + 1
                ]
        return carry

    lax.fori_loop(0, round_ref.shape[0], divide, 0)
    gather_items(
        tiles_ref, arrived_ref, round_ref, out_ref, order_ref, fields_ref, rows_ref, parts_ref
    )


def result_shape(arrived):
    slots, rows, _ = arrived.shape
    return jax.ShapeDtypeStruct((slots, rows // FIELDS * RESULTS, LANES), BF16)


def grid_step(last_tiles, last, tiles, arrived, sums):
    tile_count = sums.shape[0] - 1
    plane_size = EDGE * EDGE
    return pl.pallas_call(
        grid_kernel,
        name="grid_step",
        out_shape=(
            jax.ShapeDtypeStruct((3, tile_count, EDGE * plane_size), F32),
            jax.ShapeDtypeStruct((tile_count, 3 * EDGE, plane_size), BF16),
            result_shape(arrived),
        ),
        in_specs=[SMEM, VMEM, SMEM, VMEM, VMEM],
        out_specs=(VMEM,) * 3,
        scratch_shapes=work_shapes(arrived.shape[0], arrived.shape[1])
        + [pltpu.VMEM(sums.shape, F32)],
        compiler_params=PARAMS,
        cost_estimate=cost(10**10),
    )(last_tiles, last, tiles, arrived, sums)


def gather_step(tiles, arrived, rounded):
    return pl.pallas_call(
        gather_items,
        name="gather_step",
        out_shape=result_shape(arrived),
        in_specs=[SMEM, VMEM, VMEM],
        out_specs=VMEM,
        scratch_shapes=work_shapes(arrived.shape[0], arrived.shape[1]),
        compiler_params=PARAMS,
        cost_estimate=cost(10**10),
    )(tiles, arrived, rounded)


def unpack_kernel(dest_ref, count_ref, *refs):
    returned_refs, (velocity_ref, affine_ref) = refs[:-2], refs[-2:]
    blocks = dest_ref.shape[0]
    width = velocity_ref.shape[1] // blocks
    slots = returned_refs[0].shape[0] // HALVES
    half_width = width // HALVES
    lane = lax.broadcasted_iota(jnp.int32, (1, LANES), 1)

    def unpack(block, carry):
        dest = dest_ref[block]
        count = count_ref[block]
        for c, returned_ref in enumerate(returned_refs):

            @pl.when(dest // slots == c)
            def _():
                for h in range(HALVES):
                    rows = returned_ref[(dest - c * slots) * HALVES + h].astype(F32)
                    for q in range(half_width // LANES):
                        first = h * half_width + q * LANES
                        cols = pl.ds(pl.multiple_of(block * width + first, LANES), LANES)
                        part = jnp.where(
                            lane + first < count, rows[q * RESULTS : (q + 1) * RESULTS], 0.0
                        )
                        velocity_ref[:, cols] = part[:3]
                        affine_ref[:, cols] = part[3:]

        return carry

    lax.fori_loop(0, blocks, unpack, 0)


def unpack(dest, count, returned, width):
    particles = dest.shape[0] * width
    return pl.pallas_call(
        unpack_kernel,
        name="unpack",
        out_shape=(
            jax.ShapeDtypeStruct((3, particles), F32),
            jax.ShapeDtypeStruct((9, particles), F32),
        ),
        in_specs=[SMEM, SMEM] + [VMEM] * len(returned),
        out_specs=(VMEM, VMEM),
        compiler_params=PARAMS,
    )(dest, count, *returned)


def tile_marks(arrived):
    return arrived[:, FIELDS - 1, 0].astype(jnp.int32)


def exchange(value):
    return lax.all_to_all(value, GROUP_AXES, split_axis=0, concat_axis=0, tiled=True)


def per_device(
    particle_mass,
    particle_velocity,
    particle_affine,
    particle_cell,
    particle_fraction,
    block_owner,
    block_slot,
    block_count,
    cell_drag,
):
    group_size = lax.axis_size(GROUP_AXES)
    blocks = block_count.shape[0]
    capacity = max(1, 2 * blocks // group_size)
    chunks = 2 if capacity % 2 == 0 else 1
    portion = capacity // chunks
    payloads, dest = pack(
        chunks,
        portion,
        group_size,
        block_owner[:, 0],
        block_slot,
        block_count,
        particle_mass,
        particle_velocity,
        particle_affine,
        particle_cell,
        particle_fraction,
    )
    arrived = [exchange(payloads[0])]
    for payload in payloads[1:]:
        arrived[-1], payload = lax.optimization_barrier((arrived[-1], payload))
        arrived.append(exchange(payload))
    tiles = [tile_marks(part) for part in arrived]
    sums = start_sums(cell_drag)
    for c in range(chunks - 1):
        sums = scatter_step(tiles[c], arrived[c], sums)
    grid_velocity, rounded, results = grid_step(
        tiles[-1], arrived[-1], tiles[0], arrived[0], sums
    )
    returned = [exchange(results)]
    for c in range(1, chunks):
        returned.append(exchange(gather_step(tiles[c], arrived[c], rounded)))
    new_velocity, new_affine = unpack(
        dest, block_count, returned, particle_mass.shape[0] // blocks
    )
    return jnp.transpose(grid_velocity, (1, 0, 2)), new_velocity, new_affine


def solution(mesh):
    everywhere = ("gx", "gy", "gz")
    return jax.shard_map(
        per_device,
        mesh=mesh,
        in_specs=(
            P(everywhere),
            P(None, everywhere),
            P(None, everywhere),
            P(None, everywhere),
            P(None, everywhere),
            P(everywhere, None),
            P(everywhere),
            P(everywhere),
            P(everywhere, None),
        ),
        out_specs=(P(everywhere, None, None), P(None, everywhere), P(None, everywhere)),
        check_vma=False,
    )
```
